32 devices in a mesh: lon: 8 (over z, x), ch: 4 (over y, core).
Axes of the slice: x: 2, y: 2, z: 4, core: 2. Of those that a mesh axis runs over, the one named last changes fastest.
Arguments:
- grid_inputs: bfloat16 [230400, 474], P('lon'), may hold values from -6 to 6
- embed_weight: bfloat16 [474, 512], replicated, may hold values from -0.25 to 0.25
- embed_bias: float32 [512], replicated, may hold values from -3 to 3
- mesh_latent: bfloat16 [5120, 512], P('lon', 'ch'), may hold values from -6 to 6
- edge_features: bfloat16 [4, 180224], P(None, 'lon'), may hold values from -6 to 6
- senders: int32 [180224], P('lon'), may hold values from 0 to 230399, as said below
- receivers: int32 [180224], P('lon'), may hold values from 0 to 5119, as said below
- sender_weight: bfloat16 [512, 512], P(None, 'ch'), may hold values from -0.25 to 0.25
- receiver_weight: bfloat16 [512, 512], P(None, 'ch'), may hold values from -0.25 to 0.25
- feature_weight: bfloat16 [4, 512], P(None, 'ch'), may hold values from -3 to 3
- hidden_bias: float32 [512], P('ch'), may hold values from -3 to 3
- message_weight: bfloat16 [512, 512], P('ch'), may hold values from -0.25 to 0.25
- message_bias: float32 [512], replicated, may hold values from -1.2 to 1.2
- norm_gain: float32 [512], P('ch'), may hold values from 0.5 to 1.5
- norm_shift: float32 [512], P('ch'), may hold values from -3 to 3
Outputs:
- mesh_out: bfloat16 [5120, 512], P('lon', 'ch')
The draws below stay inside these ranges and needn't reach their ends.
Inputs may be any that keep to these rules, and one draw needn't show every extreme that they name: Edge e belongs to block b = e // 22528. Its sender is c * 640 + t with latitude row t and a column c that lies, counted around the closed circle of 360 columns, at most 4 columns before or after the block's own columns b * 45 to b * 45 + 44; some block reaches 4 columns on both sides. Within each aligned run of min(2048, 22528) edges of a block, the senders' columns, counted from the block's first widened column, lie within 7 consecutive columns. `receivers`: the receiver of edge e lies among the mesh nodes b * 640 to b * 640 + 639 of its block b = e // 22528; a mesh node may receive no edge.
All inputs are finite; a program needn't handle non-finite values.
Results may differ from the reference program's by a relative error of at most 0.0028.
Values may be sent and summed in bfloat16 or wider, within the bound.
A program may use at most 128 MiB of HBM per device.

```python
import jax
import jax.numpy as jnp
from jax import lax

CIN = 474
L = 512
CE = 4
COLS_DEV = 45
LAT = 640
M_DEV = 640
E_DEV = 22528
HALO = 4
NCOL = 360
NGRID = 230400
NMESH = 5120
NEDGE = 180224


def draw_senders(key, part):
    base_key = jax.random.fold_in(key, 11)
    reach_key, pick_key, col_key, lat_key = jax.random.split(base_key, 4)
    blocks = NEDGE // E_DEV
    reaches = jax.random.randint(reach_key, (blocks,), 1, HALO + 1)
    chosen = jax.random.randint(pick_key, (), 0, blocks)
    reaches = jnp.where(jnp.arange(blocks) == chosen, HALO, reaches)
    edge_ids = jnp.arange(NEDGE)
    owning = edge_ids // E_DEV
    within = edge_ids % E_DEV
    reach = reaches[owning]
    span = COLS_DEV + 2 * reach
    jitter = jax.random.randint(col_key, (NEDGE,), 0, 2)
    offset = jnp.minimum(within * span // E_DEV + jitter, span - 1)
    offset = jnp.where(within == 0, 0, offset)
    offset = jnp.where(within == E_DEV - 1, span - 1, offset)
    column = jnp.mod(owning * COLS_DEV + offset - reach, NCOL)
    latitude = jax.random.randint(lat_key, (NEDGE,), 0, LAT)
    return (column * LAT + latitude).astype(jnp.int32)


def draw_receivers(key, part):
    base_key = jax.random.fold_in(key, 23)
    edge_ids = jnp.arange(NEDGE)
    slots = jax.random.randint(base_key, (NEDGE,), 0, M_DEV)
    return (edge_ids // E_DEV * M_DEV + slots).astype(jnp.int32)


def shard_levels(key, extent, cuts, smallest, high):
    def one(axis_at, parts):
        steps = jax.random.uniform(jax.random.fold_in(jax.random.fold_in(key, 6), axis_at), (parts,), jnp.float32, smallest / len(cuts), high / len(cuts))
        return jnp.repeat(jnp.exp(steps), extent[axis_at] // parts).reshape((-1,) + (1,) * (len(extent) - axis_at - 1))

    level = one(*cuts[0])
    for cut in cuts[1:]:
        level = level * one(*cut)
    return level


def normal_values(own_key, shape, scale, bound, shards=(), held_as=jnp.bfloat16):
    result = scale * jax.random.normal(own_key, shape, jnp.float32)
    if shards:
        result = result * shard_levels(own_key, shape, shards, -0.22, 0.18)
    return jnp.clip(result, -bound, bound).astype(held_as)


def setup_inputs(seed: int = 0) -> dict:
    keys = jax.random.split(jax.random.key(seed), 16)
    grid_inputs = normal_values(keys[0], (NGRID, CIN), 1.0, 6.0, ((0, 8),))
    embed_weight = normal_values(keys[1], (CIN, L), CIN ** -0.5, 0.25)
    embed_bias = normal_values(keys[2], (L,), 0.5, 3.0, (), jnp.float32)
    mesh_latent = normal_values(keys[3], (NMESH, L), 1.0, 6.0, ((0, 8), (1, 4)))
    edge_features = normal_values(keys[4], (CE, NEDGE), 1.0, 6.0, ((1, 8),))
    senders = draw_senders(jax.random.fold_in(keys[15], 71), 0)
    receivers = draw_receivers(jax.random.fold_in(keys[15], 71), 0)
    sender_weight = normal_values(keys[7], (L, L), L ** -0.5, 0.25, ((1, 4),))
    receiver_weight = normal_values(keys[8], (L, L), L ** -0.5, 0.25, ((1, 4),))
    feature_weight = normal_values(keys[9], (CE, L), CE ** -0.5, 3.0, ((1, 4),))
    hidden_bias = normal_values(keys[10], (L,), 0.5, 3.0, ((0, 4),), jnp.float32)
    message_weight = normal_values(keys[11], (L, L), L ** -0.5, 0.25, ((0, 4),))
    message_bias = normal_values(keys[12], (L,), 0.2, 1.2, (), jnp.float32)
    norm_gain = jnp.clip(1.0 + 0.1 * jax.random.normal(keys[13], (L,), jnp.float32), 0.5, 1.5)
    norm_shift = normal_values(keys[14], (L,), 0.5, 3.0, ((0, 4),), jnp.float32)
    return {"grid_inputs": grid_inputs, "embed_weight": embed_weight, "embed_bias": embed_bias, "mesh_latent": mesh_latent, "edge_features": edge_features, "senders": senders, "receivers": receivers, "sender_weight": sender_weight, "receiver_weight": receiver_weight, "feature_weight": feature_weight, "hidden_bias": hidden_bias, "message_weight": message_weight, "message_bias": message_bias, "norm_gain": norm_gain, "norm_shift": norm_shift}


def reference(grid_inputs, embed_weight, embed_bias, mesh_latent, edge_features, senders, receivers, sender_weight, receiver_weight, feature_weight, hidden_bias, message_weight, message_bias, norm_gain, norm_shift):
    latent = jax.nn.silu(jnp.dot(grid_inputs, embed_weight, preferred_element_type=jnp.float32) + embed_bias).astype(jnp.bfloat16)
    sent_terms = jnp.dot(latent, sender_weight, preferred_element_type=jnp.float32)
    recv_terms = jnp.dot(mesh_latent, receiver_weight, preferred_element_type=jnp.float32)
    blocks = NEDGE // E_DEV
    feature_blocks = jnp.transpose(edge_features.reshape(CE, blocks, E_DEV), (1, 2, 0))
    send_blocks = senders.reshape(blocks, E_DEV)
    recv_blocks = receivers.reshape(blocks, E_DEV)

    def accumulate(carried, pieces):
        totals, tallies = carried
        send_ids, recv_ids, features = pieces
        before = sent_terms[send_ids] + recv_terms[recv_ids]
        before = before + jnp.dot(features, feature_weight, preferred_element_type=jnp.float32) + hidden_bias
        hidden = jax.nn.silu(before).astype(jnp.bfloat16)
        totals = totals + jax.ops.segment_sum(hidden.astype(jnp.float32), recv_ids, num_segments=NMESH)
        tallies = tallies + jax.ops.segment_sum(jnp.ones((E_DEV,), jnp.float32), recv_ids, num_segments=NMESH)
        return ((totals, tallies), None)
    start = (jnp.zeros((NMESH, L), jnp.float32), jnp.zeros((NMESH,), jnp.float32))
    (totals, tallies), ignored = lax.scan(accumulate, start, (send_blocks, recv_blocks, feature_blocks))
    aggregated = jnp.dot(totals, message_weight.astype(jnp.float32), precision=lax.Precision.HIGHEST)
    aggregated = aggregated + tallies[:, None] * message_bias
    centre = lax.optimization_barrier(jnp.mean(aggregated, axis=1, keepdims=True))
    spread = lax.optimization_barrier(jnp.mean(jnp.square(aggregated - centre), axis=1, keepdims=True))
    normed = (aggregated - centre) * lax.rsqrt(spread + 1.0)
    return (mesh_latent.astype(jnp.float32) + normed * norm_gain + norm_shift).astype(jnp.bfloat16)
```

```python
import functools

import jax
import jax.numpy as jnp
from jax import lax
from jax.experimental import pallas as pl
from jax.experimental.pallas import tpu as pltpu
from jax.sharding import PartitionSpec as P

LAT = 640
HALO = 4
CHUNK = 256


def silu(v):
    half = 0.5 * v
    return half + half * jnp.tanh(half)


def dense_kernel(x_ref, embed_ref, bias_ref, sender_ref, out_ref):
    before = (
        jnp.dot(x_ref[...], embed_ref[...], preferred_element_type=jnp.float32) + bias_ref[...]
    )
    latent = silu(before).astype(jnp.bfloat16)
    out_ref[...] = jnp.dot(
        latent, sender_ref[...], preferred_element_type=jnp.float32
    ).astype(out_ref.dtype)


def sender_terms(grid_inputs, embed_weight, embed_bias, sender_weight, rows, steps, place, dtype):
    channels, full_width = embed_weight.shape
    width = sender_weight.shape[1]
    whole = lambda shape: pl.BlockSpec(shape, lambda i: (0, 0))
    return pl.pallas_call(
        dense_kernel,
        grid=(steps,),
        in_specs=[
            pl.BlockSpec((rows, channels), lambda i: (place(i), 0)),
            whole((channels, full_width)),
            whole((1, full_width)),
            whole((full_width, width)),
        ],
        out_specs=pl.BlockSpec((rows, width), lambda i: (i, 0)),
        out_shape=jax.ShapeDtypeStruct((steps * rows, width), dtype),
        compiler_params=pltpu.CompilerParams(vmem_limit_bytes=48 << 20),
        cost_estimate=pl.CostEstimate(
            flops=2 * steps * rows * full_width * (channels + width),
            bytes_accessed=steps * rows * (2 * channels + 4 * width),
            transcendentals=steps * rows * full_width,
        ),
    )(grid_inputs, embed_weight, embed_bias.reshape(1, -1), sender_weight)


def edge_kernel(
    send_ref,
    recv_ref,
    own_ref,
    low_ref,
    high_ref,
    recv_terms_ref,
    recv_row_ref,
    features_ref,
    feature_weight_ref,
    out_ref,
    table,
    even,
    odd,
    total,
    sems,
):
    own_rows = own_ref.shape[0]
    halo_rows = low_ref.shape[0]
    pieces = ((low_ref, 0), (own_ref, halo_rows), (high_ref, halo_rows + own_rows))
    copies = [
        pltpu.make_async_copy(ref, table.at[pl.ds(at, ref.shape[0])], sems.at[n])
        for n, (ref, at) in enumerate(pieces)
    ]
    for copy in copies:
        copy.start()
    nodes = recv_terms_ref.shape[0]
    total[...] = jnp.zeros_like(total)
    for copy in copies:
        copy.wait()
    chunks = recv_row_ref.shape[1] // CHUNK
    width = recv_terms_ref.shape[1]

    def gather(chunk, held):
        base = chunk * CHUNK
        for i in range(CHUNK):
            held[pl.ds(i, 1), :] = (
                table[pl.ds(send_ref[base + i], 1), :]
                + recv_terms_ref[pl.ds(recv_ref[base + i], 1), :]
            )

    def add_up(chunk, held):
        lanes = pl.ds(pl.multiple_of(chunk * CHUNK, CHUNK), CHUNK)
        before = held[...] + lax.dot_general(
            features_ref[:, lanes],
            feature_weight_ref[...],
            (((0,), (0,)), ((), ())),
            preferred_element_type=jnp.float32,
        )
        hidden = silu(before).astype(jnp.bfloat16)
        ids = lax.broadcasted_iota(jnp.int32, (nodes, CHUNK), 0)
        one_hot = jnp.where(ids == recv_row_ref[:, lanes], 1.0, 0.0).astype(jnp.bfloat16)
        widened = jnp.concatenate([hidden, jnp.ones((CHUNK, width), jnp.bfloat16)], axis=1)
        total[...] += jnp.dot(one_hot, widened, preferred_element_type=jnp.float32)

    gather(0, even)

    def pair(n, carry):
        gather(2 * n + 1, odd)
        add_up(2 * n, even)
        gather(jnp.minimum(2 * n + 2, chunks - 1), even)
        add_up(2 * n + 1, odd)
        return carry

    lax.fori_loop(0, chunks // 2, pair, 0)
    out_ref[...] = total[...]


def node_sums(send, recv, own, low, high, recv_terms, features, feature_weight):
    edges = send.shape[0]
    nodes, width = recv_terms.shape
    table_rows = own.shape[0] + 2 * low.shape[0]
    vmem = pl.BlockSpec(memory_space=pltpu.VMEM)
    smem = pl.BlockSpec(memory_space=pltpu.SMEM)
    hbm = pl.BlockSpec(memory_space=pl.ANY)
    return pl.pallas_call(
        edge_kernel,
        in_specs=[smem, smem, hbm, hbm, hbm, vmem, vmem, vmem, vmem],
        out_specs=vmem,
        out_shape=jax.ShapeDtypeStruct((nodes, 2 * width), jnp.float32),
        scratch_shapes=[
            pltpu.VMEM((table_rows, width), jnp.float32),
            pltpu.VMEM((CHUNK, width), jnp.float32),
            pltpu.VMEM((CHUNK, width), jnp.float32),
            pltpu.VMEM((nodes, 2 * width), jnp.float32),
            pltpu.SemaphoreType.DMA((3,)),
        ],
        compiler_params=pltpu.CompilerParams(vmem_limit_bytes=48 << 20),
        cost_estimate=pl.CostEstimate(
            flops=4 * edges * nodes * width,
            bytes_accessed=4 * table_rows * width,
            transcendentals=edges * width,
        ),
    )(send, recv, own, low, high, recv_terms, recv.reshape(1, -1), features, feature_weight)


def on_device(
    grid_inputs,
    embed_weight,
    embed_bias,
    mesh_latent,
    edge_features,
    senders,
    receivers,
    sender_weight,
    receiver_weight,
    feature_weight,
    hidden_bias,
    message_weight,
    message_bias,
    norm_gain,
    norm_shift,
):
    lon_count = lax.axis_size("lon")
    lon_place = lax.axis_index("lon")
    ch_count = lax.axis_size("ch")
    ch_place = lax.axis_index("ch")
    columns = grid_inputs.shape[0] // LAT
    mesh_nodes, share_width = mesh_latent.shape
    full_width = message_weight.shape[1]

    halo_terms = sender_terms(
        grid_inputs, embed_weight, embed_bias, sender_weight, LAT, 2 * HALO,
        lambda i: jnp.where(i < HALO, i, columns - 2 * HALO + i), jnp.bfloat16,
    )
    forward = [(i, (i + 1) % lon_count) for i in range(lon_count)]
    backward = [(target, source) for source, target in forward]
    low = lax.ppermute(halo_terms[HALO * LAT:], "lon", forward)
    high = lax.ppermute(halo_terms[:HALO * LAT], "lon", backward)
    packed = jnp.concatenate([mesh_latent, message_weight.reshape(-1, share_width)], axis=0)
    gathered = lax.all_gather(packed, "ch", axis=0)
    full_mesh = jnp.swapaxes(gathered[:, :mesh_nodes], 0, 1).reshape(mesh_nodes, full_width)
    full_message = gathered[:, mesh_nodes:].reshape(full_width, full_width)

    group = max(n for n in (1, 2, 3) if columns % n == 0)
    own = sender_terms(
        grid_inputs, embed_weight, embed_bias, sender_weight, group * LAT, columns // group,
        lambda i: i, jnp.float32,
    )
    recv_terms = (
        jnp.dot(full_mesh, receiver_weight, preferred_element_type=jnp.float32) + hidden_bias
    )
    grid_column = senders // LAT
    shifted = jnp.mod(grid_column - lon_place * columns + HALO, columns * lon_count)
    local_send = shifted * LAT + senders % LAT
    local_recv = receivers - lon_place * mesh_nodes
    pad = 16 - edge_features.shape[0]
    sums = node_sums(
        local_send, local_recv, own, low.astype(jnp.float32), high.astype(jnp.float32),
        recv_terms, jnp.pad(edge_features, ((0, pad), (0, 0))),
        jnp.pad(feature_weight, ((0, pad), (0, 0))),
    )
    part = mesh_nodes // ch_count
    mine = lax.all_to_all(
        sums[:, :share_width], "ch", split_axis=0, concat_axis=1, tiled=True
    )
    tallies = lax.dynamic_slice_in_dim(sums[:, share_width:share_width + 1], ch_place * part, part, 0)
    aggregated = (
        jnp.dot(mine, full_message.astype(jnp.float32), precision=lax.Precision.HIGHEST)
        + tallies * message_bias
    )
    centre = jnp.mean(aggregated, axis=1, keepdims=True)
    spread = jnp.mean(jnp.square(aggregated - centre), axis=1, keepdims=True)
    normed = (aggregated - centre) * lax.rsqrt(spread + 1.0)
    share = lax.all_to_all(normed, "ch", split_axis=1, concat_axis=0, tiled=True)
    return (mesh_latent.astype(jnp.float32) + share * norm_gain + norm_shift).astype(jnp.bfloat16)


def solution(mesh):
    return jax.shard_map(
        on_device,
        mesh=mesh,
        in_specs=(
            P("lon", None),
            P(),
            P(),
            P("lon", "ch"),
            P(None, "lon"),
            P("lon"),
            P("lon"),
            P(None, "ch"),
            P(None, "ch"),
            P(None, "ch"),
            P("ch"),
            P("ch", None),
            P(),
            P("ch"),
            P("ch"),
        ),
        out_specs=P("lon", "ch"),
        check_vma=False,
    )
```

```python
import functools

import jax
import jax.numpy as jnp
from jax import lax
from jax.experimental import pallas as pl
from jax.experimental.pallas import tpu as pltpu
from jax.sharding import PartitionSpec as P

LAT = 640
HALO = 4
CHUNK = 256


def silu(v):
    half = 0.5 * v
    return half + half * jnp.tanh(half)


def dense_kernel(
    steps,
    x_ref,
    embed_ref,
    bias_ref,
    sender_ref,
    mesh_ref,
    message_ref,
    out_ref,
    low_ref,
    high_ref,
    mesh_all_ref,
    message_all_ref,
    first_columns,
    last_columns,
    gather_send,
    gather_recv,
    halo_send,
    halo_recv,
    local_sem,
):
    step = pl.program_id(0)
    lon_count, ch_count = lax.axis_size("lon"), lax.axis_size("ch")
    lon_place, ch_place = lax.axis_index("lon"), lax.axis_index("ch")
    right = lax.rem(lon_place + 1, lon_count)
    left = lax.rem(lon_place + lon_count - 1, lon_count)
    halo_rows = low_ref.shape[0]
    pairs = ((mesh_ref, mesh_all_ref), (message_ref, message_all_ref))
    local = [
        pltpu.make_async_copy(ref, all_ref.at[ch_place], local_sem.at[n])
        for n, (ref, all_ref) in enumerate(pairs)
    ]
    partners = [lax.rem(ch_place + j, ch_count) for j in range(1, ch_count)]
    gathers = [
        pltpu.make_async_remote_copy(
            src_ref=ref,
            dst_ref=all_ref.at[ch_place],
            send_sem=gather_send.at[n, j],
            recv_sem=gather_recv.at[n, j],
            device_id={"ch": partner},
            device_id_type=pl.DeviceIdType.MESH,
        )
        for n, (ref, all_ref) in enumerate(pairs)
        for j, partner in enumerate(partners)
    ]
    halos = [
        pltpu.make_async_remote_copy(
            src_ref=src,
            dst_ref=dst,
            send_sem=halo_send.at[n],
            recv_sem=halo_recv.at[n],
            device_id={"lon": side},
            device_id_type=pl.DeviceIdType.MESH,
        )
        for n, (src, dst, side) in enumerate(
            ((last_columns, low_ref, right), (first_columns, high_ref, left))
        )
    ]

    @pl.when(step == 0)
    def _():
        barrier = pltpu.get_barrier_semaphore()
        for partner in partners:
            pl.semaphore_signal(
                barrier, inc=1, device_id={"ch": partner}, device_id_type=pl.DeviceIdType.MESH
            )
        for side in (left, right):
            pl.semaphore_signal(
                barrier, inc=1, device_id={"lon": side}, device_id_type=pl.DeviceIdType.MESH
            )
        pl.semaphore_wait(barrier, ch_count + 1)
        for copy in gathers + local:
            copy.start()

    @pl.when(step == 2)
    def _():
        for copy in halos:
            copy.start()

    before = (
        lax.dot_general(
            x_ref[...], embed_ref[...], (((0,), (0,)), ((), ())),
            preferred_element_type=jnp.float32,
        )
        + bias_ref[...]
    )
    latent = silu(before).astype(jnp.bfloat16)
    out_ref[...] = jnp.dot(latent, sender_ref[...], preferred_element_type=jnp.float32)

    @pl.when(step == 0)
    def _():
        first_columns[...] = out_ref[:halo_rows, :].astype(jnp.bfloat16)

    @pl.when(step == 1)
    def _():
        last_columns[...] = out_ref[out_ref.shape[0] - halo_rows:, :].astype(jnp.bfloat16)

    @pl.when(step == steps - 1)
    def _():
        for copy in gathers + halos + local:
            copy.wait()


def sender_terms(
    grid_inputs, embed_weight, embed_bias, sender_weight, mesh_latent, message_weight
):
    channels, full_width = embed_weight.shape
    width = sender_weight.shape[1]
    points = grid_inputs.shape[0]
    columns = points // LAT
    group = max(n for n in range(1, 6) if columns % n == 0)
    steps = columns // group
    assert group >= HALO and steps > 2
    rows = group * LAT
    ch_count = lax.axis_size("ch")

    def place(i):
        return jnp.where(i == 1, steps - 1, jnp.maximum(i - 1, 0))

    whole = lambda shape: pl.BlockSpec(shape, lambda i: (0, 0))
    hbm = pl.BlockSpec(memory_space=pl.ANY)
    halo = (HALO * LAT, width)
    return pl.pallas_call(
        functools.partial(dense_kernel, steps),
        grid=(steps,),
        in_specs=[
            pl.BlockSpec((channels, rows), lambda i: (0, place(i))),
            whole((channels, full_width)),
            whole((1, full_width)),
            whole((full_width, width)),
            hbm,
            hbm,
        ],
        out_specs=[pl.BlockSpec((rows, width), lambda i: (place(i), 0)), hbm, hbm, hbm, hbm],
        out_shape=[
            jax.ShapeDtypeStruct((points, width), jnp.float32),
            jax.ShapeDtypeStruct(halo, jnp.bfloat16),
            jax.ShapeDtypeStruct(halo, jnp.bfloat16),
            jax.ShapeDtypeStruct((ch_count, *mesh_latent.shape), jnp.bfloat16),
            jax.ShapeDtypeStruct((ch_count, *message_weight.shape), jnp.bfloat16),
        ],
        scratch_shapes=[
            pltpu.VMEM(halo, jnp.bfloat16),
            pltpu.VMEM(halo, jnp.bfloat16),
            pltpu.SemaphoreType.DMA((2, ch_count - 1)),
            pltpu.SemaphoreType.DMA((2, ch_count - 1)),
            pltpu.SemaphoreType.DMA((2,)),
            pltpu.SemaphoreType.DMA((2,)),
            pltpu.SemaphoreType.DMA((2,)),
        ],
        compiler_params=pltpu.CompilerParams(
            vmem_limit_bytes=56 << 20, collective_id=0, has_side_effects=True
        ),
        cost_estimate=pl.CostEstimate(
            flops=2 * points * full_width * (channels + width),
            bytes_accessed=points * (2 * channels + 4 * width),
            transcendentals=points * full_width,
        ),
    )(grid_inputs.T, embed_weight, embed_bias.reshape(1, -1), sender_weight,
      mesh_latent, message_weight)


def edge_kernel(
    send_ref,
    recv_ref,
    own_ref,
    low_ref,
    high_ref,
    mesh_all_ref,
    receiver_ref,
    hidden_bias_ref,
    recv_row_ref,
    features_ref,
    feature_weight_ref,
    out_ref,
    table,
    recv_terms_ref,
    even,
    odd,
    total,
    sem,
):
    own_rows = own_ref.shape[0]
    halo_rows = low_ref.shape[0]
    copy = pltpu.make_async_copy(own_ref, table.at[pl.ds(halo_rows, own_rows)], sem)
    copy.start()
    table[:halo_rows, :] = low_ref[...].astype(jnp.float32)
    table[halo_rows + own_rows:, :] = high_ref[...].astype(jnp.float32)
    parts, nodes, part_width = mesh_all_ref.shape
    recv_terms_ref[...] = hidden_bias_ref[...] + sum(
        jnp.dot(
            mesh_all_ref[n],
            receiver_ref[n * part_width:(n + 1) * part_width, :],
            preferred_element_type=jnp.float32,
        )
        for n in range(parts)
    )
    total[...] = jnp.zeros_like(total)
    copy.wait()
    chunks = recv_row_ref.shape[1] // CHUNK
    width = recv_terms_ref.shape[1]

    def gather(chunk, held):
        base = chunk * CHUNK
        for i in range(CHUNK):
            held[pl.ds(i, 1), :] = (
                table[pl.ds(send_ref[base + i], 1), :]
                + recv_terms_ref[pl.ds(recv_ref[base + i], 1), :]
            )

    def add_up(chunk, held):
        lanes = pl.ds(pl.multiple_of(chunk * CHUNK, CHUNK), CHUNK)
        before = held[...] + lax.dot_general(
            features_ref[:, lanes],
            feature_weight_ref[...],
            (((0,), (0,)), ((), ())),
            preferred_element_type=jnp.float32,
        )
        hidden = silu(before).astype(jnp.bfloat16)
        ids = lax.broadcasted_iota(jnp.int32, (nodes, CHUNK), 0)
        one_hot = jnp.where(ids == recv_row_ref[:, lanes], 1.0, 0.0).astype(jnp.bfloat16)
        widened = jnp.concatenate([hidden, jnp.ones((CHUNK, width), jnp.bfloat16)], axis=1)
        total[...] += jnp.dot(one_hot, widened, preferred_element_type=jnp.float32)

    gather(0, even)

    def pair(n, carry):
        gather(2 * n + 1, odd)
        add_up(2 * n, even)
        gather(jnp.minimum(2 * n + 2, chunks - 1), even)
        add_up(2 * n + 1, odd)
        return carry

    lax.fori_loop(0, chunks // 2, pair, 0)
    out_ref[...] = total[...]


def node_sums(
    send, recv, own, low, high, mesh_all, receiver_weight, hidden_bias, features, feature_weight
):
    edges = send.shape[0]
    parts, nodes, width = mesh_all.shape
    table_rows = own.shape[0] + 2 * low.shape[0]
    vmem = pl.BlockSpec(memory_space=pltpu.VMEM)
    smem = pl.BlockSpec(memory_space=pltpu.SMEM)
    hbm = pl.BlockSpec(memory_space=pl.ANY)
    return pl.pallas_call(
        edge_kernel,
        in_specs=[smem, smem, hbm] + [vmem] * 8,
        out_specs=vmem,
        out_shape=jax.ShapeDtypeStruct((nodes, 2 * width), jnp.float32),
        scratch_shapes=[
            pltpu.VMEM((table_rows, width), jnp.float32),
            pltpu.VMEM((nodes, width), jnp.float32),
            pltpu.VMEM((CHUNK, width), jnp.float32),
            pltpu.VMEM((CHUNK, width), jnp.float32),
            pltpu.VMEM((nodes, 2 * width), jnp.float32),
            pltpu.SemaphoreType.DMA,
        ],
        compiler_params=pltpu.CompilerParams(vmem_limit_bytes=48 << 20),
        cost_estimate=pl.CostEstimate(
            flops=4 * edges * nodes * width,
            bytes_accessed=4 * table_rows * width,
            transcendentals=edges * width,
        ),
    )(send, recv, own, low, high, mesh_all, receiver_weight, hidden_bias.reshape(1, -1),
      recv.reshape(1, -1), features, feature_weight)


def on_device(
    grid_inputs,
    embed_weight,
    embed_bias,
    mesh_latent,
    edge_features,
    senders,
    receivers,
    sender_weight,
    receiver_weight,
    feature_weight,
    hidden_bias,
    message_weight,
    message_bias,
    norm_gain,
    norm_shift,
):
    lon_count = lax.axis_size("lon")
    lon_place = lax.axis_index("lon")
    ch_count = lax.axis_size("ch")
    ch_place = lax.axis_index("ch")
    columns = grid_inputs.shape[0] // LAT
    mesh_nodes, share_width = mesh_latent.shape
    full_width = message_weight.shape[1]

    own, low, high, mesh_all, message_all = sender_terms(
        grid_inputs, embed_weight, embed_bias, sender_weight, mesh_latent, message_weight
    )
    full_message = message_all.reshape(full_width, full_width)
    grid_column = senders // LAT
    shifted = jnp.mod(grid_column - lon_place * columns + HALO, columns * lon_count)
    local_send = shifted * LAT + senders % LAT
    local_recv = receivers - lon_place * mesh_nodes
    pad = 16 - edge_features.shape[0]
    sums = node_sums(
        local_send, local_recv, own, low, high, mesh_all, receiver_weight, hidden_bias,
        jnp.pad(edge_features, ((0, pad), (0, 0))),
        jnp.pad(feature_weight, ((0, pad), (0, 0))),
    )
    part = mesh_nodes // ch_count
    mine = lax.all_to_all(
        sums[:, :share_width], "ch", split_axis=0, concat_axis=1, tiled=True
    )
    tallies = lax.dynamic_slice_in_dim(sums[:, share_width:share_width + 1], ch_place * part, part, 0)
    aggregated = (
        jnp.dot(mine, full_message.astype(jnp.float32), precision=lax.Precision.HIGHEST)
        + tallies * message_bias
    )
    centre = jnp.mean(aggregated, axis=1, keepdims=True)
    spread = jnp.mean(jnp.square(aggregated - centre), axis=1, keepdims=True)
    normed = (aggregated - centre) * lax.rsqrt(spread + 1.0)
    share = lax.all_to_all(normed, "ch", split_axis=1, concat_axis=0, tiled=True)
    return (mesh_latent.astype(jnp.float32) + share * norm_gain + norm_shift).astype(jnp.bfloat16)


def solution(mesh):
    return jax.shard_map(
        on_device,
        mesh=mesh,
        in_specs=(
            P("lon", None),
            P(),
            P(),
            P("lon", "ch"),
            P(None, "lon"),
            P("lon"),
            P("lon"),
            P(None, "ch"),
            P(None, "ch"),
            P(None, "ch"),
            P("ch"),
            P("ch", None),
            P(),
            P("ch"),
            P("ch"),
        ),
        out_specs=P("lon", "ch"),
        check_vma=False,
    )
```

```python
import functools

import jax
import jax.numpy as jnp
from jax import lax
from jax.experimental import pallas as pl
from jax.experimental.pallas import tpu as pltpu
from jax.sharding import PartitionSpec as P

LAT = 640
HALO = 4
CHUNK = 256


def silu(v):
    half = 0.5 * v
    return half + half * jnp.tanh(half)


def dense_kernel(
    steps,
    x_ref,
    embed_ref,
    bias_ref,
    sender_ref,
    mesh_ref,
    message_ref,
    out_ref,
    low_ref,
    high_ref,
    mesh_all_ref,
    message_all_ref,
    first_columns,
    last_columns,
    gather_send,
    gather_recv,
    halo_send,
    halo_recv,
    local_sem,
):
    step = pl.program_id(0)
    lon_count, ch_count = lax.axis_size("lon"), lax.axis_size("ch")
    lon_place, ch_place = lax.axis_index("lon"), lax.axis_index("ch")
    right = lax.rem(lon_place + 1, lon_count)
    left = lax.rem(lon_place + lon_count - 1, lon_count)
    halo_rows = low_ref.shape[0]
    pairs = ((mesh_ref, mesh_all_ref), (message_ref, message_all_ref))
    local = [
        pltpu.make_async_copy(ref, all_ref.at[ch_place], local_sem.at[n])
        for n, (ref, all_ref) in enumerate(pairs)
    ]
    partners = [lax.rem(ch_place + j, ch_count) for j in range(1, ch_count)]
    gathers = [
        pltpu.make_async_remote_copy(
            src_ref=ref,
            dst_ref=all_ref.at[ch_place],
            send_sem=gather_send.at[n, j],
            recv_sem=gather_recv.at[n, j],
            device_id={"ch": partner},
            device_id_type=pl.DeviceIdType.MESH,
        )
        for n, (ref, all_ref) in enumerate(pairs)
        for j, partner in enumerate(partners)
    ]
    halos = [
        pltpu.make_async_remote_copy(
            src_ref=src,
            dst_ref=dst,
            send_sem=halo_send.at[n],
            recv_sem=halo_recv.at[n],
            device_id={"lon": side},
            device_id_type=pl.DeviceIdType.MESH,
        )
        for n, (src, dst, side) in enumerate(
            ((first_columns, high_ref, left), (last_columns, low_ref, right))
        )
    ]

    @pl.when(step == 0)
    def _():
        barrier = pltpu.get_barrier_semaphore()
        for partner in partners:
            pl.semaphore_signal(
                barrier, inc=1, device_id={"ch": partner}, device_id_type=pl.DeviceIdType.MESH
            )
        for side in (left, right):
            pl.semaphore_signal(
                barrier, inc=1, device_id={"lon": side}, device_id_type=pl.DeviceIdType.MESH
            )
        pl.semaphore_wait(barrier, ch_count + 1)
        for copy in gathers + local:
            copy.start()

    for n, copy in enumerate(halos):
        pl.when(step == n + 1)(copy.start)

    before = (
        lax.dot_general(
            x_ref[...], embed_ref[...], (((0,), (0,)), ((), ())),
            preferred_element_type=jnp.float32,
        )
        + bias_ref[...]
    )
    latent = silu(before).astype(jnp.bfloat16)
    out_ref[...] = jnp.dot(latent, sender_ref[...], preferred_element_type=jnp.float32)

    @pl.when(step == 0)
    def _():
        first_columns[...] = out_ref[:halo_rows, :].astype(jnp.bfloat16)

    @pl.when(step == 1)
    def _():
        last_columns[...] = out_ref[out_ref.shape[0] - halo_rows:, :].astype(jnp.bfloat16)

    @pl.when(step == steps - 1)
    def _():
        for copy in gathers + halos + local:
            copy.wait()


def sender_terms(
    grid_inputs, embed_weight, embed_bias, sender_weight, mesh_latent, message_weight
):
    channels, full_width = embed_weight.shape
    width = sender_weight.shape[1]
    points = grid_inputs.shape[0]
    columns = points // LAT
    group = max(n for n in range(1, 6) if columns % n == 0)
    steps = columns // group
    assert group >= HALO and steps > 2
    rows = group * LAT
    ch_count = lax.axis_size("ch")

    def place(i):
        return jnp.where(i == 1, steps - 1, jnp.maximum(i - 1, 0))

    whole = lambda shape: pl.BlockSpec(shape, lambda i: (0, 0))
    hbm = pl.BlockSpec(memory_space=pl.ANY)
    halo = (HALO * LAT, width)
    return pl.pallas_call(
        functools.partial(dense_kernel, steps),
        grid=(steps,),
        in_specs=[
            pl.BlockSpec((channels, rows), lambda i: (0, place(i))),
            whole((channels, full_width)),
            whole((1, full_width)),
            whole((full_width, width)),
            hbm,
            hbm,
        ],
        out_specs=[pl.BlockSpec((rows, width), lambda i: (place(i), 0)), hbm, hbm, hbm, hbm],
        out_shape=[
            jax.ShapeDtypeStruct((points, width), jnp.float32),
            jax.ShapeDtypeStruct(halo, jnp.bfloat16),
            jax.ShapeDtypeStruct(halo, jnp.bfloat16),
            jax.ShapeDtypeStruct((ch_count, *mesh_latent.shape), jnp.bfloat16),
            jax.ShapeDtypeStruct((ch_count, *message_weight.shape), jnp.bfloat16),
        ],
        scratch_shapes=[
            pltpu.VMEM(halo, jnp.bfloat16),
            pltpu.VMEM(halo, jnp.bfloat16),
            pltpu.SemaphoreType.DMA((2, ch_count - 1)),
            pltpu.SemaphoreType.DMA((2, ch_count - 1)),
            pltpu.SemaphoreType.DMA((2,)),
            pltpu.SemaphoreType.DMA((2,)),
            pltpu.SemaphoreType.DMA((2,)),
        ],
        compiler_params=pltpu.CompilerParams(
            vmem_limit_bytes=56 << 20, collective_id=0, has_side_effects=True
        ),
        cost_estimate=pl.CostEstimate(
            flops=2 * points * full_width * (channels + width),
            bytes_accessed=points * (2 * channels + 4 * width),
            transcendentals=points * full_width,
        ),
    )(grid_inputs.T, embed_weight, embed_bias.reshape(1, -1), sender_weight,
      mesh_latent, message_weight)


def edge_kernel(
    send_ref,
    recv_ref,
    own_ref,
    low_ref,
    high_ref,
    mesh_all_ref,
    receiver_ref,
    hidden_bias_ref,
    recv_row_ref,
    features_ref,
    feature_weight_ref,
    out_ref,
    tally_ref,
    table,
    recv_terms_ref,
    even,
    odd,
    total,
    sem,
):
    own_rows = own_ref.shape[0]
    halo_rows = low_ref.shape[0]
    copy = pltpu.make_async_copy(own_ref, table.at[pl.ds(halo_rows, own_rows)], sem)
    copy.start()
    table[:halo_rows, :] = low_ref[...].astype(jnp.float32)
    table[halo_rows + own_rows:, :] = high_ref[...].astype(jnp.float32)
    parts, nodes, part_width = mesh_all_ref.shape
    recv_terms_ref[...] = hidden_bias_ref[...] + sum(
        jnp.dot(
            mesh_all_ref[n],
            receiver_ref[n * part_width:(n + 1) * part_width, :],
            preferred_element_type=jnp.float32,
        )
        for n in range(parts)
    )
    total[...] = jnp.zeros_like(total)
    copy.wait()
    chunks = recv_row_ref.shape[1] // CHUNK
    width = recv_terms_ref.shape[1]

    def gather(chunk, held):
        base = chunk * CHUNK
        for i in range(CHUNK):
            held[pl.ds(i, 1), :] = (
                table[pl.ds(send_ref[base + i], 1), :]
                + recv_terms_ref[pl.ds(recv_ref[base + i], 1), :]
            )

    def add_up(chunk, held):
        lanes = pl.ds(pl.multiple_of(chunk * CHUNK, CHUNK), CHUNK)
        before = held[...] + lax.dot_general(
            features_ref[:, lanes],
            feature_weight_ref[...],
            (((0,), (0,)), ((), ())),
            preferred_element_type=jnp.float32,
        )
        hidden = silu(before).astype(jnp.bfloat16)
        ids = lax.broadcasted_iota(jnp.int32, (nodes, CHUNK), 0)
        one_hot = jnp.where(ids == recv_row_ref[:, lanes], 1.0, 0.0).astype(jnp.bfloat16)
        widened = jnp.concatenate([hidden, jnp.ones((CHUNK, width), jnp.bfloat16)], axis=1)
        total[...] += jnp.dot(one_hot, widened, preferred_element_type=jnp.float32)

    gather(0, even)

    def pair(n, carry):
        gather(2 * n + 1, odd)
        add_up(2 * n, even)
        gather(jnp.minimum(2 * n + 2, chunks - 1), even)
        add_up(2 * n + 1, odd)
        return carry

    lax.fori_loop(0, chunks // 2, pair, 0)
    out_ref[...] = total[:, :width]
    tally_ref[...] = total[:, width:]


def node_sums(
    send, recv, own, low, high, mesh_all, receiver_weight, hidden_bias, features, feature_weight
):
    edges = send.shape[0]
    parts, nodes, width = mesh_all.shape
    table_rows = own.shape[0] + 2 * low.shape[0]
    vmem = pl.BlockSpec(memory_space=pltpu.VMEM)
    smem = pl.BlockSpec(memory_space=pltpu.SMEM)
    hbm = pl.BlockSpec(memory_space=pl.ANY)
    return pl.pallas_call(
        edge_kernel,
        in_specs=[smem, smem, hbm] + [vmem] * 8,
        out_specs=[vmem, vmem],
        out_shape=[jax.ShapeDtypeStruct((nodes, width), jnp.float32)] * 2,
        scratch_shapes=[
            pltpu.VMEM((table_rows, width), jnp.float32),
            pltpu.VMEM((nodes, width), jnp.float32),
            pltpu.VMEM((CHUNK, width), jnp.float32),
            pltpu.VMEM((CHUNK, width), jnp.float32),
            pltpu.VMEM((nodes, 2 * width), jnp.float32),
            pltpu.SemaphoreType.DMA,
        ],
        compiler_params=pltpu.CompilerParams(vmem_limit_bytes=48 << 20),
        cost_estimate=pl.CostEstimate(
            flops=4 * edges * nodes * width,
            bytes_accessed=4 * table_rows * width,
            transcendentals=edges * width,
        ),
    )(send, recv, own, low, high, mesh_all, receiver_weight, hidden_bias.reshape(1, -1),
      recv.reshape(1, -1), features, feature_weight)


def tail_kernel(
    totals_ref,
    tally_ref,
    message_ref,
    message_bias_ref,
    latent_ref,
    gain_ref,
    shift_ref,
    out_ref,
    got,
    give,
    back,
    there_send,
    there_recv,
    back_send,
    back_recv,
):
    ch_count = lax.axis_size("ch")
    me = lax.axis_index("ch")
    parts, part, width = got.shape
    partners = [lax.rem(me + j, ch_count) for j in range(1, ch_count)]
    barrier = pltpu.get_barrier_semaphore()
    for partner in partners:
        pl.semaphore_signal(
            barrier, inc=1, device_id={"ch": partner}, device_id_type=pl.DeviceIdType.MESH
        )
    pl.semaphore_wait(barrier, ch_count - 1)

    def copy_to(source, target, sends, recvs, j, partner):
        return pltpu.make_async_remote_copy(
            src_ref=source,
            dst_ref=target.at[me],
            send_sem=sends.at[j],
            recv_sem=recvs.at[j],
            device_id={"ch": partner},
            device_id_type=pl.DeviceIdType.MESH,
        )

    there = [
        copy_to(totals_ref.at[partner], got, there_send, there_recv, j, partner)
        for j, partner in enumerate(partners)
    ]
    for copy in there:
        copy.start()
    got[me] = totals_ref[me]
    bias = tally_ref[me][:, :1] * message_bias_ref[...]
    for copy in there:
        copy.wait()
    aggregated = bias
    for n in range(parts):
        rest = got[n]
        for _ in range(3):
            piece = rest.astype(jnp.bfloat16)
            aggregated += jnp.dot(piece, message_ref[n], preferred_element_type=jnp.float32)
            rest = rest - piece.astype(jnp.float32)
    centre = jnp.mean(aggregated, axis=1, keepdims=True)
    spread = jnp.mean(jnp.square(aggregated - centre), axis=1, keepdims=True)
    normed = (aggregated - centre) * lax.rsqrt(spread + 1.0)
    for n in range(parts):
        give[n] = normed[:, n * width:(n + 1) * width]
    back[me] = give[me]
    returns = [
        copy_to(give.at[partner], back, back_send, back_recv, j, partner)
        for j, partner in enumerate(partners)
    ]
    for copy in returns:
        copy.start()
    for copy in returns:
        copy.wait()
    for n in range(parts):
        rows = slice(n * part, (n + 1) * part)
        out_ref[rows, :] = (
            latent_ref[rows, :].astype(jnp.float32) + back[n] * gain_ref[...] + shift_ref[...]
        ).astype(out_ref.dtype)


def finished(totals, tallies, message_all, message_bias, mesh_latent, norm_gain, norm_shift):
    nodes, width = mesh_latent.shape
    ch_count = lax.axis_size("ch")
    blocks = (ch_count, nodes // ch_count, width)
    vmem = pl.BlockSpec(memory_space=pltpu.VMEM)
    return pl.pallas_call(
        tail_kernel,
        in_specs=[vmem] * 7,
        out_specs=vmem,
        out_shape=jax.ShapeDtypeStruct((nodes, width), jnp.bfloat16),
        scratch_shapes=[pltpu.VMEM(blocks, jnp.float32)] * 3
        + [pltpu.SemaphoreType.DMA((ch_count - 1,))] * 4,
        compiler_params=pltpu.CompilerParams(
            vmem_limit_bytes=32 << 20, collective_id=1, has_side_effects=True
        ),
    )(totals.reshape(blocks), tallies.reshape(blocks), message_all, message_bias.reshape(1, -1),
      mesh_latent, norm_gain.reshape(1, -1), norm_shift.reshape(1, -1))


def on_device(
    grid_inputs,
    embed_weight,
    embed_bias,
    mesh_latent,
    edge_features,
    senders,
    receivers,
    sender_weight,
    receiver_weight,
    feature_weight,
    hidden_bias,
    message_weight,
    message_bias,
    norm_gain,
    norm_shift,
):
    lon_count = lax.axis_size("lon")
    lon_place = lax.axis_index("lon")
    columns = grid_inputs.shape[0] // LAT
    mesh_nodes = mesh_latent.shape[0]

    own, low, high, mesh_all, message_all = sender_terms(
        grid_inputs, embed_weight, embed_bias, sender_weight, mesh_latent, message_weight
    )
    grid_column = senders // LAT
    shifted = jnp.mod(grid_column - lon_place * columns + HALO, columns * lon_count)
    local_send = shifted * LAT + senders % LAT
    local_recv = receivers - lon_place * mesh_nodes
    pad = 16 - edge_features.shape[0]
    totals, tallies = node_sums(
        local_send, local_recv, own, low, high, mesh_all, receiver_weight, hidden_bias,
        jnp.pad(edge_features, ((0, pad), (0, 0))),
        jnp.pad(feature_weight, ((0, pad), (0, 0))),
    )
    return finished(
        totals, tallies, message_all, message_bias, mesh_latent, norm_gain, norm_shift
    )


def solution(mesh):
    return jax.shard_map(
        on_device,
        mesh=mesh,
        in_specs=(
            P("lon", None),
            P(),
            P(),
            P("lon", "ch"),
            P(None, "lon"),
            P("lon"),
            P("lon"),
            P(None, "ch"),
            P(None, "ch"),
            P(None, "ch"),
            P("ch"),
            P("ch", None),
            P(),
            P("ch"),
            P("ch"),
        ),
        out_specs=P("lon", "ch"),
        check_vma=False,
    )
```
